256 devices in a mesh: blk: 128 (over z, y, x_lo, core), head: 2 (over x_hi).
Axes of the slice: x: 4 (x_hi: 2, x_lo: 2; x = x_hi * 2 + x_lo), y: 4, z: 8, core: 2. Of those that a mesh axis runs over, the one named last changes fastest.
Arguments:
- queries: bfloat16 [65536, 16, 128], P('blk', 'head'), may hold values from -6 to 6
- out_grad: bfloat16 [65536, 16, 128], P('blk', 'head'), may hold values from -6 to 6
- outputs: bfloat16 [65536, 16, 128], P('blk', 'head'), may hold values from -6 to 6
- key_vectors: bfloat16 [65536, 128], P('blk'), may hold values from -6 to 6
- value_vectors: bfloat16 [65536, 128], P('blk'), may hold values from -6 to 6
- logsumexp: float32 [65536, 16], P('blk', 'head'), may hold values from 4 to 7
- positions: int32 [65536], P('blk'), may hold values from 0 to 65535, as said below
- doc_start: int32 [65536], P('blk'), may hold values from 0 to 65535, as said below
Outputs:
- query_grad: bfloat16 [65536, 16, 128], P('blk', 'head')
- key_grad: bfloat16 [65536, 128], P('blk')
- value_grad: bfloat16 [65536, 128], P('blk')
The draws below stay inside these ranges and needn't reach their ends.
Inputs may be any that keep to these rules, and one draw needn't show every extreme that they name: positions is a permutation of 0 to 65535; row r holds position (r mod 512) * 128 + sigma(r div 512), sigma a permutation of the blocks of 512 rows. doc_start of a row is the first position of the document that holds the row's position; documents are runs of consecutive positions, the first starting at 0, and the last position starts a document of its own.
All inputs are finite; a program needn't handle non-finite values.
Results may differ from the reference program's by a relative error of at most 0.0063.
Values may be sent and summed in bfloat16 or wider, within the bound.
A program may use at most 64 MiB of HBM per device.

```python
import jax
import jax.numpy as jnp
from jax import lax

HQ = 16
HD = 128
TOK_DEV = 512
STEPS = 4
SEQ = 65536
N_BLK = 128


def shared_positions(key):
    sub_key = jax.random.fold_in(key, 11)
    block_order = jax.random.permutation(sub_key, N_BLK).astype(jnp.int32)
    row_ids = jnp.arange(SEQ, dtype=jnp.int32)
    return (row_ids % TOK_DEV * N_BLK + block_order[row_ids // TOK_DEV]).astype(jnp.int32)


def draw_positions(key, part):
    return shared_positions(key)


def draw_doc_start(key, part):
    places = shared_positions(key)
    doc_flags = jax.random.randint(jax.random.fold_in(key, 12), (SEQ,), 0, max(SEQ // 8, 2)) == 0
    cell_ids = jnp.arange(SEQ, dtype=jnp.int32)
    start_marks = jnp.where(doc_flags | (cell_ids == 0) | (cell_ids == SEQ - 1), cell_ids, 0).astype(jnp.int32)
    doc_starts = lax.cummax(start_marks, axis=0)
    return doc_starts[places].astype(jnp.int32)


def levels(key, shape, pieces, least, high):
    level, own = 1.0, jax.random.fold_in(key, 6)
    for axis_at, shards_of in pieces:
        steps = jnp.exp(jax.random.uniform(jax.random.fold_in(own, axis_at), (shards_of,), jnp.float32, least / len(pieces), high / len(pieces)))
        level = level * jnp.repeat(steps, shape[axis_at] // shards_of).reshape([-1 if axis == axis_at else 1 for axis in range(len(shape))])
    return level


def normal_values(rng, extent, width, reach, cuts=(), kind=jnp.bfloat16):
    result = width * jax.random.normal(rng, extent, jnp.float32)
    if cuts:
        result = result * levels(rng, extent, cuts, -0.22, 0.18)
    return jnp.clip(result, -reach, reach).astype(kind)


def setup_inputs(seed: int = 0) -> dict:
    key_of = jax.random.split(jax.random.key(seed), 9)
    return {
        "queries": normal_values(key_of[0], (SEQ, HQ, HD), 1.0, 6.0, ((0, 128), (1, 2))),
        "out_grad": normal_values(key_of[1], (SEQ, HQ, HD), 1.0, 6.0, ((0, 128), (1, 2))),
        "outputs": normal_values(key_of[2], (SEQ, HQ, HD), 1.0, 6.0, ((0, 128), (1, 2))),
        "key_vectors": normal_values(key_of[3], (SEQ, HD), 1.0, 6.0, ((0, 128),)),
        "value_vectors": normal_values(key_of[4], (SEQ, HD), 1.0, 6.0, ((0, 128),)),
        "logsumexp": jnp.clip(4.0 + 3.0 * jax.random.uniform(key_of[5], (SEQ, HQ), jnp.float32) ** levels(key_of[5], (SEQ, HQ), ((0, 128), (1, 2)), -0.2, 0.2), 4.0, 7.0),
        "positions": draw_positions(jax.random.fold_in(key_of[8], 71), 0),
        "doc_start": draw_doc_start(jax.random.fold_in(key_of[8], 71), 0),
    }


def block_grads(queries, out_grad, logsumexp, row_delta, query_places, query_starts, key_vectors, value_vectors, key_places):
    scaling = HD ** -0.5
    query_wide = queries.astype(jnp.float32)
    grad_wide = out_grad.astype(jnp.float32)
    key_wide = key_vectors.astype(jnp.float32)
    value_wide = value_vectors.astype(jnp.float32)
    scores = jnp.einsum("thd,kd->htk", query_wide, key_wide) * scaling
    allowed = (key_places[None, :] <= query_places[:, None]) & (key_places[None, :] >= query_starts[:, None])
    attend = jnp.where(allowed[None], jnp.exp(scores - logsumexp.T[:, :, None]), jnp.float32(0.0))
    attend_low = lax.optimization_barrier(attend.astype(jnp.bfloat16)).astype(jnp.float32)
    attend_grad = jnp.einsum("thd,kd->htk", grad_wide, value_wide)
    score_grad = attend * (attend_grad - row_delta.T[:, :, None])
    score_low = lax.optimization_barrier(score_grad.astype(jnp.bfloat16)).astype(jnp.float32)
    value_part = jnp.einsum("htk,thd->kd", attend_low, grad_wide)
    key_part = scaling * jnp.einsum("htk,thd->kd", score_low, query_wide)
    query_part = scaling * jnp.einsum("htk,kd->thd", score_low, key_wide)
    return query_part, key_part, value_part


def reference(queries, out_grad, outputs, key_vectors, value_vectors, logsumexp, positions, doc_start):
    row_delta = jnp.sum(out_grad.astype(jnp.float32) * outputs.astype(jnp.float32), axis=-1)
    query_blocks = queries.reshape(N_BLK, TOK_DEV, HQ, HD)
    grad_blocks = out_grad.reshape(N_BLK, TOK_DEV, HQ, HD)
    norm_blocks = logsumexp.reshape(N_BLK, TOK_DEV, HQ)
    delta_blocks = row_delta.reshape(N_BLK, TOK_DEV, HQ)
    place_blocks = positions.reshape(N_BLK, TOK_DEV)
    start_blocks = doc_start.reshape(N_BLK, TOK_DEV)
    key_blocks = key_vectors.reshape(N_BLK, TOK_DEV, HD)
    value_blocks = value_vectors.reshape(N_BLK, TOK_DEV, HD)
    query_total = jnp.zeros((N_BLK, TOK_DEV, HQ, HD), jnp.float32)
    key_total = jnp.zeros((N_BLK, TOK_DEV, HD), jnp.float32)
    value_total = jnp.zeros((N_BLK, TOK_DEV, HD), jnp.float32)

    def block_pass(inputs):
        return block_grads(*inputs)

    for cycle_step in range(STEPS):
        moved_keys = jnp.roll(key_blocks, -cycle_step, axis=0)
        moved_values = jnp.roll(value_blocks, -cycle_step, axis=0)
        moved_places = jnp.roll(place_blocks, -cycle_step, axis=0)
        query_part, key_part, value_part = lax.map(block_pass, (query_blocks, grad_blocks, norm_blocks, delta_blocks, place_blocks, start_blocks, moved_keys, moved_values, moved_places))
        query_total = query_total + query_part
        key_total = key_total + jnp.roll(key_part, cycle_step, axis=0)
        value_total = value_total + jnp.roll(value_part, cycle_step, axis=0)
    return (query_total.reshape(SEQ, HQ, HD).astype(jnp.bfloat16), key_total.reshape(SEQ, HD).astype(jnp.bfloat16), value_total.reshape(SEQ, HD).astype(jnp.bfloat16))
```

```python
import functools
import math

import jax
import jax.numpy as jnp
from jax import lax
from jax.experimental import pallas as pl
from jax.experimental.pallas import tpu as pltpu
from jax.sharding import PartitionSpec as P

MESH = pl.DeviceIdType.MESH
STEPS = 4
TOK = 512
HEADS = 8
HD = 128
ROWS = TOK * HEADS
CHUNK = 512
N_CHUNK = ROWS // CHUNK
TILE = 128
EXP2 = math.log2(math.e)
SCALE = HD**-0.5


def tiles_of(chunk):
    last = (chunk + 1) * CHUNK // HEADS
    return -(-last // TILE)


def scores_of(chunk, qdo, weights, sdp):
    width = 2 * TILE * tiles_of(chunk)
    sdp[:, :width] = jnp.dot(
        qdo[chunk * CHUNK : (chunk + 1) * CHUNK, :],
        weights[:, :width],
        preferred_element_type=jnp.float32,
    )


def attend_of(chunk, sdp, lse_b, delta_b, start_b, width_b, key_pos, p_out, d_out):
    piece = 64
    for at in range(0, CHUNK, piece):
        here = slice(at, at + piece)
        rows = slice(chunk * CHUNK + at, chunk * CHUNK + at + piece)
        lse, delta = lse_b[rows, :], delta_b[rows, :]
        start, width = start_b[rows, :], width_b[rows, :]
        for j in range(tiles_of(chunk)):
            keys = slice(j * TILE, (j + 1) * TILE)
            s = sdp[here, 2 * j * TILE : (2 * j + 1) * TILE]
            dp = sdp[here, (2 * j + 1) * TILE : (2 * j + 2) * TILE]
            after = (key_pos[j : j + 1, :] - start).astype(jnp.uint32)
            p = jnp.where(after <= width, jnp.exp2(s * (SCALE * EXP2) - lse), 0.0)
            p_out[here, keys] = p.astype(jnp.bfloat16)
            d_out[here, keys] = (p * (dp - delta)).astype(jnp.bfloat16)


def grads_of(chunk, p_in, d_in, qdo_t, keys, acc, dq):
    nk = tiles_of(chunk) * TILE
    rows = slice(chunk * CHUNK, (chunk + 1) * CHUNK)
    acc[HD:, :nk] += jnp.dot(qdo_t[HD:, rows], p_in[:, :nk], preferred_element_type=jnp.float32)
    acc[:HD, :nk] += jnp.dot(qdo_t[:HD, rows], d_in[:, :nk], preferred_element_type=jnp.float32)
    dq[rows, :] += jnp.dot(d_in[:, :nk], keys[:nk, :], preferred_element_type=jnp.float32)


def kernel(
    comm,
    n_blk,
    pos_smem,
    start_smem,
    q_hbm,
    do_hbm,
    o_hbm,
    k_hbm,
    v_hbm,
    lse_hbm,
    pos_hbm,
    dq_out,
    dk_out,
    dv_out,
    qdo,
    o_buf,
    lse_in,
    kv,
    pos,
    qdo_t,
    lse_b,
    delta_b,
    start_b,
    width_b,
    weights,
    sdp_a,
    sdp_b,
    p_a,
    p_b,
    d_a,
    d_b,
    acc,
    dq,
    dq_low,
    grad_low,
    part,
    inbox,
    load_sem,
    kv_send,
    kv_recv,
    pos_send,
    pos_recv,
    part_send,
    part_recv,
    out_sem,
):
    if comm:
        blk, head = lax.axis_index("blk"), lax.axis_index("head")
    else:
        blk, head = 0, 0
    odd = lax.rem(blk, 2) == 1 if comm else None

    def device(shift):
        return (lax.rem(blk + shift + n_blk, n_blk), head)

    loads = [
        pltpu.make_async_copy(k_hbm, kv.at[0, 0:TOK, :], load_sem.at[0]),
        pltpu.make_async_copy(v_hbm, kv.at[0, TOK : 2 * TOK, :], load_sem.at[1]),
        pltpu.make_async_copy(pos_hbm, pos.at[0], load_sem.at[2]),
        pltpu.make_async_copy(do_hbm, qdo.at[:, HD : 2 * HD], load_sem.at[3]),
        pltpu.make_async_copy(o_hbm, o_buf, load_sem.at[4]),
        pltpu.make_async_copy(q_hbm, qdo.at[:, 0:HD], load_sem.at[5]),
        pltpu.make_async_copy(lse_hbm, lse_in, load_sem.at[6]),
    ]
    for load in loads:
        load.start()

    def kv_copy(src, dst, send, shift):
        to = device(shift)
        return (
            pltpu.make_async_remote_copy(
                kv.at[src], kv.at[dst], kv_send.at[send], kv_recv.at[dst], to, MESH
            ),
            pltpu.make_async_remote_copy(
                pos.at[src], pos.at[dst], pos_send.at[send], pos_recv.at[dst], to, MESH
            ),
        )

    def start_kv(*args):
        for copy in kv_copy(*args):
            copy.start()

    def wait_kv_send(*args):
        for copy in kv_copy(*args):
            copy.wait_send()

    def part_copy(src, dst, shift):
        return pltpu.make_async_remote_copy(
            part.at[src], inbox.at[dst], part_send.at[src], part_recv.at[dst], device(shift), MESH
        )

    twin = (blk, 1 - head)

    if comm:
        barrier = pltpu.get_barrier_semaphore()
        for shift in (-3, -2, -1, 1, 2, 3):
            pl.semaphore_signal(barrier, inc=1, device_id=device(shift), device_id_type=MESH)
        pl.semaphore_signal(barrier, inc=1, device_id=twin, device_id_type=MESH)
        pl.semaphore_wait(barrier, 7)
    for load in loads[:3]:
        load.wait()
    if comm:
        start_kv(0, 1, 0, -1)

    def spread(t, carry):
        first = start_smem[t]
        at = pl.multiple_of(t * HEADS, HEADS)
        start_b[pl.ds(at, HEADS), :] = jnp.full((HEADS, TILE), first, jnp.int32)
        width_b[pl.ds(at, HEADS), :] = jnp.full(
            (HEADS, TILE), pos_smem[t] - first, jnp.int32
        ).astype(jnp.uint32)
        return carry

    lax.fori_loop(0, TOK, spread, 0, unroll=8)

    weights[...] = jnp.zeros_like(weights)

    loads[6].wait()
    lse_t = jnp.swapaxes(lse_in[...], 0, 1) * EXP2
    for t in range(TOK):
        lse_b[t * HEADS : (t + 1) * HEADS, :] = jnp.broadcast_to(
            lse_t[:, t : t + 1], (HEADS, TILE)
        )

    for load in loads[3:6]:
        load.wait()

    def prepare(i, carry):
        rows = pl.ds(pl.multiple_of(i * 256, 256), 256)
        grad = qdo[rows, HD:]
        delta = jnp.sum(
            grad.astype(jnp.float32) * o_buf[rows, :].astype(jnp.float32), axis=1, keepdims=True
        )
        delta_b[rows, :] = jnp.broadcast_to(delta, (256, TILE))
        qdo_t[HD:, rows] = jnp.swapaxes(grad, 0, 1)
        qdo_t[:HD, rows] = jnp.swapaxes(qdo[rows, :HD], 0, 1)
        return carry

    lax.fori_loop(0, ROWS // 256, prepare, 0)
    dq[...] = jnp.zeros_like(dq)

    def step(turn, carry):
        slot = lax.rem(turn + 1, STEPS)
        if comm:

            @pl.when(turn < STEPS - 1)
            def _():
                for copy in kv_copy(slot, slot, 0, 0):
                    copy.wait_recv()

            @pl.when(jnp.logical_and(turn == 0, odd))
            def _():
                start_kv(0, 2, 1, -2)
                start_kv(1, 2, 2, -1)

            @pl.when(jnp.logical_and(turn == 1, odd))
            def _():
                start_kv(2, 3, 3, -1)

            @pl.when(jnp.logical_and(turn == 1, jnp.logical_not(odd)))
            def _():
                start_kv(0, 3, 1, -3)

        keys = kv.at[slot, 0:TOK, :]
        values = kv.at[slot, TOK : 2 * TOK, :]
        key_pos = pos[slot]
        for j in range(TOK // TILE):
            rows = slice(j * TILE, (j + 1) * TILE)
            at = 2 * j * TILE
            weights[:HD, at : at + TILE] = jnp.swapaxes(keys[rows, :], 0, 1)
            weights[HD:, at + TILE : at + 2 * TILE] = jnp.swapaxes(values[rows, :], 0, 1)
        acc[...] = jnp.zeros_like(acc)
        sdp, p_bf, d_bf = (sdp_a, sdp_b), (p_a, p_b), (d_a, d_b)
        for c in range(-1, N_CHUNK + 1):
            if c + 1 < N_CHUNK:
                scores_of(c + 1, qdo, weights, sdp[(c + 1) % 2])
            if 0 <= c < N_CHUNK:
                attend_of(
                    c, sdp[c % 2], lse_b, delta_b, start_b, width_b, key_pos, p_bf[c % 2], d_bf[c % 2]
                )
            if c >= 1:
                grads_of(c - 1, p_bf[(c - 1) % 2], d_bf[(c - 1) % 2], qdo_t, keys, acc, dq)

        if comm:

            @pl.when(turn == 0)
            def _():
                part[0] = acc[...].astype(jnp.bfloat16)

                @pl.when(odd)
                def _():
                    part_copy(0, 0, -1).start()

                @pl.when(jnp.logical_not(odd))
                def _():
                    part_copy(0, 2, 1).start()

            @pl.when(turn == 1)
            def _():
                @pl.when(odd)
                def _():
                    part[1] = acc[...].astype(jnp.bfloat16)
                    part_copy(1, 1, -1).start()

                @pl.when(jnp.logical_not(odd))
                def _():
                    part_copy(0, 0, 0).wait_recv()
                    part[1] = (acc[...] + inbox[0].astype(jnp.float32)).astype(jnp.bfloat16)
                    part_copy(1, 2, 2).start()

            @pl.when(turn == 2)
            def _():
                @pl.when(odd)
                def _():
                    part[2] = acc[...].astype(jnp.bfloat16)

                @pl.when(jnp.logical_not(odd))
                def _():
                    part_copy(0, 1, 0).wait_recv()
                    part[2] = (acc[...] + inbox[1].astype(jnp.float32)).astype(jnp.bfloat16)

                part_copy(2, 3, 3).start()

        return carry

    lax.fori_loop(0, STEPS, step, 0)

    twin_copy = pltpu.make_async_remote_copy(
        part.at[3], inbox.at[4], part_send.at[3], part_recv.at[4], twin, MESH
    )
    if comm:
        part_copy(0, 2, 0).wait_recv()
        part_copy(0, 3, 0).wait_recv()
        part[3] = (
            acc[...] + inbox[2].astype(jnp.float32) + inbox[3].astype(jnp.float32)
        ).astype(jnp.bfloat16)
        twin_copy.start()
    else:
        part[3] = acc[...].astype(jnp.bfloat16)
    for i in range(N_CHUNK):
        rows = slice(i * CHUNK, (i + 1) * CHUNK)
        dq_low[rows, :] = (dq[rows, :] * SCALE).astype(jnp.bfloat16)
    outs = [pltpu.make_async_copy(dq_low, dq_out, out_sem.at[0])]
    outs[0].start()
    if comm:
        twin_copy.wait_recv()
        total = part[3].astype(jnp.float32) + inbox[4].astype(jnp.float32)
    else:
        total = part[3].astype(jnp.float32)
    grad_low[0] = jnp.swapaxes(total[:HD] * SCALE, 0, 1).astype(jnp.bfloat16)
    grad_low[1] = jnp.swapaxes(total[HD:], 0, 1).astype(jnp.bfloat16)
    outs.append(pltpu.make_async_copy(grad_low.at[0], dk_out, out_sem.at[1]))
    outs.append(pltpu.make_async_copy(grad_low.at[1], dv_out, out_sem.at[2]))
    outs[1].start()
    outs[2].start()
    if comm:
        wait_kv_send(0, 1, 0, -1)

        @pl.when(odd)
        def _():
            wait_kv_send(0, 2, 1, -2)
            wait_kv_send(1, 2, 2, -1)
            wait_kv_send(2, 3, 3, -1)
            part_copy(0, 0, -1).wait_send()
            part_copy(1, 1, -1).wait_send()

        @pl.when(jnp.logical_not(odd))
        def _():
            wait_kv_send(0, 3, 1, -3)
            part_copy(0, 2, 1).wait_send()
            part_copy(1, 2, 2).wait_send()

        part_copy(2, 3, 3).wait_send()
        twin_copy.wait_send()
    for out in outs:
        out.wait()


def call(comm, n_blk, q, do, o, k, v, lse, pos, start):
    any_space = pl.BlockSpec(memory_space=pl.ANY)
    smem = pl.BlockSpec(memory_space=pltpu.SMEM)
    flat = (ROWS, HD)
    low, full = jnp.bfloat16, jnp.float32
    dq, dk, dv = pl.pallas_call(
        functools.partial(kernel, comm, n_blk),
        out_shape=(
            jax.ShapeDtypeStruct(flat, low),
            jax.ShapeDtypeStruct(k.shape, low),
            jax.ShapeDtypeStruct(v.shape, low),
        ),
        in_specs=[smem, smem] + [any_space] * 7,
        out_specs=(any_space,) * 3,
        scratch_shapes=[
            pltpu.VMEM((ROWS, 2 * HD), low),
            pltpu.VMEM(flat, low),
            pltpu.VMEM((TOK, HEADS), full),
            pltpu.VMEM((STEPS, 2 * TOK, HD), low),
            pltpu.VMEM((STEPS, TOK // TILE, TILE), jnp.int32),
            pltpu.VMEM((2 * HD, ROWS), low),
            pltpu.VMEM(flat, full),
            pltpu.VMEM(flat, full),
            pltpu.VMEM(flat, jnp.int32),
            pltpu.VMEM(flat, jnp.uint32),
            pltpu.VMEM((2 * HD, 2 * TOK), low),
            pltpu.VMEM((CHUNK, 2 * TOK), full),
            pltpu.VMEM((CHUNK, 2 * TOK), full),
            pltpu.VMEM((CHUNK, TOK), low),
            pltpu.VMEM((CHUNK, TOK), low),
            pltpu.VMEM((CHUNK, TOK), low),
            pltpu.VMEM((CHUNK, TOK), low),
            pltpu.VMEM((2 * HD, TOK), full),
            pltpu.VMEM(flat, full),
            pltpu.VMEM(flat, low),
            pltpu.VMEM((2, TOK, HD), low),
            pltpu.VMEM((4, 2 * HD, TOK), low),
            pltpu.VMEM((5, 2 * HD, TOK), low),
            pltpu.SemaphoreType.DMA((7,)),
            pltpu.SemaphoreType.DMA((4,)),
            pltpu.SemaphoreType.DMA((4,)),
            pltpu.SemaphoreType.DMA((4,)),
            pltpu.SemaphoreType.DMA((4,)),
            pltpu.SemaphoreType.DMA((4,)),
            pltpu.SemaphoreType.DMA((5,)),
            pltpu.SemaphoreType.DMA((3,)),
        ],
        compiler_params=pltpu.CompilerParams(
            collective_id=0 if comm else None,
            has_side_effects=True,
            vmem_limit_bytes=56 * 1024 * 1024,
        ),
    )(
        pos,
        start,
        q.reshape(flat),
        do.reshape(flat),
        o.reshape(flat),
        k,
        v,
        lse,
        pos.reshape(TOK // TILE, TILE),
    )
    return dq.reshape(q.shape), dk, dv


def solution(mesh):
    n_blk = mesh.shape["blk"]
    in_specs = (
        P("blk", "head", None),
        P("blk", "head", None),
        P("blk", "head", None),
        P("blk", None),
        P("blk", None),
        P("blk", "head"),
        P("blk"),
        P("blk"),
    )
    out_specs = (P("blk", "head", None), P("blk", None), P("blk", None))
    return jax.shard_map(
        functools.partial(call, True, n_blk),
        mesh=mesh,
        in_specs=in_specs,
        out_specs=out_specs,
        check_vma=False,
    )
```

```python
import functools
import math

import jax
import jax.numpy as jnp
from jax import lax
from jax.experimental import pallas as pl
from jax.experimental.pallas import tpu as pltpu
from jax.sharding import PartitionSpec as P

MESH = pl.DeviceIdType.MESH
STEPS = 4
TOK = 512
HEADS = 8
HD = 128
ROWS = TOK * HEADS
CHUNK = 512
N_CHUNK = ROWS // CHUNK
TILE = 128
EXP2 = math.log2(math.e)
SCALE = HD**-0.5
HALF = 0.5
MATE, BESIDE = 0, 1
NEAR, FAR, TWIN = 0, 2, 4


def tiles_of(chunk):
    last = (chunk + 1) * CHUNK // HEADS
    return -(-last // TILE)


def scores_of(chunk, qdo, weights, sdp):
    width = 2 * TILE * tiles_of(chunk)
    sdp[:, :width] = jnp.dot(
        qdo[chunk * CHUNK : (chunk + 1) * CHUNK, :],
        weights[:, :width],
        preferred_element_type=jnp.float32,
    )


def attend_of(chunk, sdp, lse_b, delta_b, start_b, place_b, key_pos, p_out, d_out):
    piece = 64
    for at in range(0, CHUNK, piece):
        here = slice(at, at + piece)
        rows = slice(chunk * CHUNK + at, chunk * CHUNK + at + piece)
        lse, delta = lse_b[rows, :], delta_b[rows, :]
        start = start_b[rows, :]
        for j in range(tiles_of(chunk)):
            keys = slice(j * TILE, (j + 1) * TILE)
            s = sdp[here, 2 * j * TILE : (2 * j + 1) * TILE]
            dp = sdp[here, (2 * j + 1) * TILE : (2 * j + 2) * TILE]
            at_key = key_pos[j : j + 1, :]
            met = at_key >= start
            if (j + 1) * TILE * HEADS > chunk * CHUNK:
                met = jnp.logical_and(met, at_key <= place_b[rows, :])
            p = jnp.where(met, jnp.exp2(s * (SCALE * EXP2) - lse), 0.0)
            p_out[here, keys] = p.astype(jnp.bfloat16)
            d_out[here, keys] = (p * (dp - delta)).astype(jnp.bfloat16)


def grads_of(chunk, p_in, d_in, qdo_t, keys, acc, dq):
    nk = tiles_of(chunk) * TILE
    rows = slice(chunk * CHUNK, (chunk + 1) * CHUNK)
    acc[1, :, :nk] += jnp.dot(qdo_t[HD:, rows], p_in[:, :nk], preferred_element_type=jnp.float32)
    acc[0, :, :nk] += jnp.dot(qdo_t[:HD, rows], d_in[:, :nk], preferred_element_type=jnp.float32)
    dq[rows, :] += jnp.dot(d_in[:, :nk], keys[:nk, :], preferred_element_type=jnp.float32)


def kernel(
    n_blk,
    pos_in,
    start_in,
    q_hbm,
    do_hbm,
    o_hbm,
    k_hbm,
    v_hbm,
    lse_hbm,
    pos_hbm,
    dq_out,
    dk_out,
    dv_out,
    pos_smem,
    start_smem,
    qdo,
    o_buf,
    lse_in,
    kv,
    pos,
    qdo_t,
    lse_b,
    delta_b,
    start_b,
    place_b,
    weights,
    sdp_a,
    sdp_b,
    p_a,
    p_b,
    d_a,
    d_b,
    acc,
    own,
    dq,
    grad_low,
    part,
    inbox,
    mate_box,
    load_sem,
    kv_send,
    kv_recv,
    pos_send,
    pos_recv,
    part_send,
    part_recv,
    mate_recv,
    last_sem,
):
    blk, head = lax.axis_index("blk"), lax.axis_index("head")
    odd = lax.rem(blk, 2) == 1
    even = jnp.logical_not(odd)

    reach = jnp.where(odd, 2, 3)

    def device(shift, across=0):
        return (lax.rem(blk + shift + n_blk, n_blk), lax.rem(head + across, 2))

    barrier = pltpu.get_barrier_semaphore()

    def greet(*where):
        for shift, across in where:
            pl.semaphore_signal(
                barrier, inc=1, device_id=device(shift, across), device_id_type=MESH
            )

    @pl.when(odd)
    def _():
        greet((1, 0), (2, 0), (3, 0), (-1, 0), (-2, 0), (-2, 1), (0, 1))

    @pl.when(even)
    def _():
        greet((1, 0), (-2, 0), (-2, 1), (-3, 0), (-3, 1), (0, 1))

    loads = [
        pltpu.make_async_copy(k_hbm, kv.at[0, 0:TOK, :], load_sem.at[0]),
        pltpu.make_async_copy(v_hbm, kv.at[0, TOK : 2 * TOK, :], load_sem.at[1]),
        pltpu.make_async_copy(pos_hbm, pos.at[0], load_sem.at[2]),
        pltpu.make_async_copy(pos_in, pos_smem, load_sem.at[7]),
        pltpu.make_async_copy(start_in, start_smem, load_sem.at[8]),
        pltpu.make_async_copy(lse_hbm, lse_in, load_sem.at[3]),
        pltpu.make_async_copy(do_hbm, qdo.at[:, HD : 2 * HD], load_sem.at[4]),
        pltpu.make_async_copy(q_hbm, qdo.at[:, 0:HD], load_sem.at[5]),
        pltpu.make_async_copy(o_hbm, o_buf, load_sem.at[6]),
    ]
    for load in loads:
        load.start()

    def kv_copy(src, dst, send, shift):
        to = device(shift)
        return (
            pltpu.make_async_remote_copy(
                kv.at[src], kv.at[dst], kv_send.at[send], kv_recv.at[dst], to, MESH
            ),
            pltpu.make_async_remote_copy(
                pos.at[src], pos.at[dst], pos_send.at[send], pos_recv.at[dst], to, MESH
            ),
        )

    def start_kv(*args):
        for copy in kv_copy(*args):
            copy.start()

    def wait_kv_send(*args):
        for copy in kv_copy(*args):
            copy.wait_send()

    def wait_kv(slot):
        for copy in kv_copy(slot, slot, 0, 0):
            copy.wait_recv()

    def part_copy(src, dst, shift, across=0):
        return pltpu.make_async_remote_copy(
            part.at[src, lax.rem(head + across, 2)],
            inbox.at[dst],
            part_send.at[src, across],
            part_recv.at[dst],
            device(shift, across),
            MESH,
        )

    def mate_copy(src, dst, shift):
        return pltpu.make_async_remote_copy(
            part.at[src],
            mate_box.at[dst],
            part_send.at[src, 0],
            mate_recv.at[dst],
            device(shift),
            MESH,
        )

    def wait_part(dst):
        part_copy(0, dst, 0).wait_recv()

    def wait_mate(dst):
        mate_copy(0, dst, 0).wait_recv()

    def send_halves(src, dst, shift):
        part_copy(src, dst, shift).start()
        part_copy(src, dst + 1, shift, 1).start()

    def low(x):
        return x.astype(jnp.bfloat16)

    def full(x):
        return x.astype(jnp.float32)

    @pl.when(even)
    def _():
        for load in loads[:3]:
            load.wait()
        pl.semaphore_wait(barrier, 6)
        start_kv(0, 1, 0, -1)

    def spread(t, carry):
        at = pl.multiple_of(t * HEADS, HEADS)
        start_b[pl.ds(at, HEADS), :] = jnp.full((HEADS, TILE), start_smem[t], jnp.int32)
        place_b[pl.ds(at, HEADS), :] = jnp.full((HEADS, TILE), pos_smem[t], jnp.int32)
        return carry

    loads[3].wait()
    loads[4].wait()
    lax.fori_loop(0, TOK, spread, 0, unroll=16)
    weights[...] = jnp.zeros_like(weights)
    loads[5].wait()
    lse_t = lse_in[...] * EXP2
    for t in range(TOK):
        lse_b[t * HEADS : (t + 1) * HEADS, :] = jnp.broadcast_to(
            lse_t[:, t : t + 1], (HEADS, TILE)
        )
    @pl.when(odd)
    def _():
        for load in loads[:3]:
            load.wait()
        pl.semaphore_wait(barrier, 7)
        start_kv(0, 1, 0, -1)

    for load in loads[6:]:
        load.wait()

    def prepare(i, carry):
        rows = pl.ds(pl.multiple_of(i * 512, 512), 512)
        grad = qdo[rows, HD:]
        delta = jnp.sum(
            grad.astype(jnp.float32) * o_buf[rows, :].astype(jnp.float32), axis=1, keepdims=True
        )
        delta_b[rows, :] = jnp.broadcast_to(delta, (512, TILE))
        qdo_t[HD:, rows] = jnp.swapaxes(grad, 0, 1)
        qdo_t[:HD, rows] = jnp.swapaxes(qdo[rows, :HD], 0, 1)
        return carry

    lax.fori_loop(0, ROWS // 512, prepare, 0)
    dq[...] = jnp.zeros_like(dq)

    def work(slot):
        keys = kv.at[slot, 0:TOK, :]
        values = kv.at[slot, TOK : 2 * TOK, :]
        key_pos = pos[slot]
        for j in range(TOK // TILE):
            rows = slice(j * TILE, (j + 1) * TILE)
            at = 2 * j * TILE
            weights[:HD, at : at + TILE] = jnp.swapaxes(keys[rows, :], 0, 1)
            weights[HD:, at + TILE : at + 2 * TILE] = jnp.swapaxes(values[rows, :], 0, 1)
        acc[...] = jnp.zeros_like(acc)
        sdp, p_bf, d_bf = (sdp_a, sdp_b), (p_a, p_b), (d_a, d_b)
        for c in range(-1, N_CHUNK + 1):
            if c + 1 < N_CHUNK:
                scores_of(c + 1, qdo, weights, sdp[(c + 1) % 2])
            if 0 <= c < N_CHUNK:
                attend_of(
                    c, sdp[c % 2], lse_b, delta_b, start_b, place_b, key_pos, p_bf[c % 2], d_bf[c % 2]
                )
            if c >= 1:
                grads_of(c - 1, p_bf[(c - 1) % 2], d_bf[(c - 1) % 2], qdo_t, keys, acc, dq)

    def step(turn, carry):
        slot = jnp.where(jnp.logical_and(odd, turn > 1), 5 - turn, turn)

        @pl.when(turn == 1)
        def _():
            wait_kv(1)

        @pl.when(jnp.logical_and(turn == 1, odd))
        def _():
            start_kv(1, 2, 2, -1)

        @pl.when(jnp.logical_and(turn == 2, odd))
        def _():
            wait_kv(2)
            start_kv(2, 3, 3, -1)
            wait_kv(3)

        @pl.when(jnp.logical_and(turn == 2, even))
        def _():
            wait_kv(2)

        @pl.when(jnp.logical_and(turn == 3, even))
        def _():
            wait_kv(3)

        @pl.when(jnp.logical_and(turn == 3, odd))
        def _():
            wait_mate(BESIDE)
            own[...] += full(mate_box[BESIDE])
            part[3] = low(own[...])
            part_copy(3, TWIN, 0, 1).start()

        work(slot)

        @pl.when(turn == 0)
        def _():
            start_kv(0, reach, 1, -reach)
            own[...] = acc[...]

        @pl.when(jnp.logical_and(turn == 0, even))
        def _():
            part[3] = low(own[...])
            part_copy(3, TWIN, 0, 1).start()

        @pl.when(turn == 1)
        def _():
            part[0] = low(acc[...])

        @pl.when(jnp.logical_and(turn == 1, odd))
        def _():
            mate_copy(0, MATE, -1).start()

        @pl.when(jnp.logical_and(turn == 1, even))
        def _():
            mate_copy(0, BESIDE, 1).start()

        @pl.when(jnp.logical_and(turn == 2, odd))
        def _():
            part[1] = low(acc[...])
            send_halves(1, FAR, 3)

        @pl.when(jnp.logical_and(turn == 2, even))
        def _():
            wait_mate(MATE)
            part[1] = low(acc[...] + full(mate_box[MATE]))
            send_halves(1, NEAR, 2)

        @pl.when(jnp.logical_and(turn == 3, odd))
        def _():
            wait_mate(MATE)
            part[2] = low(acc[...] + full(mate_box[MATE]))
            send_halves(2, FAR, 2)

        @pl.when(jnp.logical_and(turn == 3, even))
        def _():
            part[2] = low(acc[...])
            mate_copy(2, MATE, 1).start()

        return carry

    lax.fori_loop(0, STEPS, step, 0)

    for i in range(N_CHUNK):
        rows = slice(i * CHUNK, (i + 1) * CHUNK)
        dq_out[rows, :] = (dq[rows, :] * (SCALE * HALF)).astype(jnp.bfloat16)

    wait_part(TWIN)
    half = own.at[head]
    half[...] += full(inbox[TWIN])

    @pl.when(even)
    def _():
        wait_part(NEAR)
        wait_part(NEAR + 1)
        half[...] += full(inbox[NEAR]) + full(inbox[NEAR + 1])

    wait_part(FAR)
    wait_part(FAR + 1)
    total = half[...] + (full(inbox[FAR]) + full(inbox[FAR + 1]))
    factor = jnp.where(head == 0, SCALE * HALF, HALF)
    grad_low[head] = low(jnp.swapaxes(total * factor, 0, 1))
    last = pltpu.make_async_remote_copy(
        grad_low.at[head], grad_low.at[head], last_sem.at[0], last_sem.at[1], device(0, 1), MESH
    )
    last.start()
    last.wait()
    dk_out[...] = grad_low[0]
    dv_out[...] = grad_low[1]

    def sent(src, dst, shift, across=0):
        part_copy(src, dst, shift, across).wait_send()

    sent(3, TWIN, 0, 1)
    wait_kv_send(0, 1, 0, -1)
    wait_kv_send(0, reach, 1, -reach)

    @pl.when(odd)
    def _():
        wait_kv_send(1, 2, 2, -1)
        wait_kv_send(2, 3, 3, -1)
        mate_copy(0, MATE, -1).wait_send()
        sent(1, FAR, 3)
        sent(1, FAR + 1, 3, 1)
        sent(2, FAR, 2)
        sent(2, FAR + 1, 2, 1)

    @pl.when(even)
    def _():
        mate_copy(0, BESIDE, 1).wait_send()
        sent(1, NEAR, 2)
        sent(1, NEAR + 1, 2, 1)
        mate_copy(2, MATE, 1).wait_send()


def call(n_blk, q, do, o, k, v, lse, pos, start):
    in_hbm = pl.BlockSpec(memory_space=pltpu.HBM)
    flat = (ROWS, HD)
    low, full = jnp.bfloat16, jnp.float32
    dq, dk, dv = pl.pallas_call(
        functools.partial(kernel, n_blk),
        out_shape=(
            pltpu.VMEM(flat, low),
            pltpu.VMEM(k.shape, low),
            pltpu.VMEM(v.shape, low),
        ),
        in_specs=[in_hbm] * 9,
        out_specs=(pl.BlockSpec(memory_space=pltpu.VMEM),) * 3,
        scratch_shapes=[
            pltpu.SMEM((TOK,), jnp.int32),
            pltpu.SMEM((TOK,), jnp.int32),
            pltpu.VMEM((ROWS, 2 * HD), low),
            pltpu.VMEM(flat, low),
            pltpu.VMEM((HEADS, TOK), full),
            pltpu.VMEM((STEPS, 2 * TOK, HD), low),
            pltpu.VMEM((STEPS, TOK // TILE, TILE), jnp.int32),
            pltpu.VMEM((2 * HD, ROWS), low),
            pltpu.VMEM(flat, full),
            pltpu.VMEM(flat, full),
            pltpu.VMEM(flat, jnp.int32),
            pltpu.VMEM(flat, jnp.int32),
            pltpu.VMEM((2 * HD, 2 * TOK), low),
            pltpu.VMEM((CHUNK, 2 * TOK), full),
            pltpu.VMEM((CHUNK, 2 * TOK), full),
            pltpu.VMEM((CHUNK, TOK), low),
            pltpu.VMEM((CHUNK, TOK), low),
            pltpu.VMEM((CHUNK, TOK), low),
            pltpu.VMEM((CHUNK, TOK), low),
            pltpu.VMEM((2, HD, TOK), full),
            pltpu.VMEM((2, HD, TOK), full),
            pltpu.VMEM(flat, full),
            pltpu.VMEM((2, TOK, HD), low),
            pltpu.VMEM((4, 2, HD, TOK), low),
            pltpu.VMEM((5, HD, TOK), low),
            pltpu.VMEM((2, 2, HD, TOK), low),
            pltpu.SemaphoreType.DMA((9,)),
            pltpu.SemaphoreType.DMA((4,)),
            pltpu.SemaphoreType.DMA((4,)),
            pltpu.SemaphoreType.DMA((4,)),
            pltpu.SemaphoreType.DMA((4,)),
            pltpu.SemaphoreType.DMA((4, 2)),
            pltpu.SemaphoreType.DMA((5,)),
            pltpu.SemaphoreType.DMA((2,)),
            pltpu.SemaphoreType.DMA((2,)),
        ],
        compiler_params=pltpu.CompilerParams(
            collective_id=0,
            has_side_effects=True,
            vmem_limit_bytes=125 * 512 * 1024,
        ),
    )(
        pos,
        start,
        q.reshape(flat),
        do.reshape(flat),
        o.reshape(flat),
        k,
        v,
        lse.T,
        pos.reshape(TOK // TILE, TILE),
    )
    return dq.reshape(q.shape) * 2, dk * 2, dv * 2


def solution(mesh):
    n_blk = mesh.shape["blk"]
    in_specs = (
        P("blk", "head", None),
        P("blk", "head", None),
        P("blk", "head", None),
        P("blk", None),
        P("blk", None),
        P("blk", "head"),
        P("blk"),
        P("blk"),
    )
    out_specs = (P("blk", "head", None), P("blk", None), P("blk", None))
    return jax.shard_map(
        functools.partial(call, n_blk),
        mesh=mesh,
        in_specs=in_specs,
        out_specs=out_specs,
        check_vma=False,
    )
```

```python
import functools
import math

import jax
import jax.numpy as jnp
from jax import lax
from jax.experimental import pallas as pl
from jax.experimental.pallas import tpu as pltpu
from jax.sharding import PartitionSpec as P

MESH = pl.DeviceIdType.MESH
STEPS = 4
TOK = 512
HEADS = 8
HD = 128
ROWS = TOK * HEADS
CHUNK = 512
N_CHUNK = ROWS // CHUNK
TILE = 128
EXP2 = math.log2(math.e)
SCALE = HD**-0.5
HALF = 0.5
MATE, BESIDE = 0, 1
NEAR, FAR, TWIN = 0, 2, 4


def tiles_of(chunk):
    last = (chunk + 1) * CHUNK // HEADS
    return -(-last // TILE)


def scores_of(chunk, qdo, weights, sdp):
    width = 2 * TILE * tiles_of(chunk)
    sdp[:, :width] = jnp.dot(
        qdo[chunk * CHUNK : (chunk + 1) * CHUNK, :],
        weights[:, :width],
        preferred_element_type=jnp.float32,
    )


def attend_of(chunk, sdp, lse_b, delta_b, start_b, place_b, key_pos, p_out, d_out):
    piece = 64
    for at in range(0, CHUNK, piece):
        here = slice(at, at + piece)
        rows = slice(chunk * CHUNK + at, chunk * CHUNK + at + piece)
        lse, delta = lse_b[rows, :], delta_b[rows, :]
        start = start_b[rows, :]
        for j in range(tiles_of(chunk)):
            keys = slice(j * TILE, (j + 1) * TILE)
            s = sdp[here, 2 * j * TILE : (2 * j + 1) * TILE]
            dp = sdp[here, (2 * j + 1) * TILE : (2 * j + 2) * TILE]
            at_key = key_pos[j : j + 1, :]
            met = at_key >= start
            if (j + 1) * TILE * HEADS > chunk * CHUNK:
                met = jnp.logical_and(met, at_key <= place_b[rows, :])
            p = jnp.where(met, jnp.exp2(s * (SCALE * EXP2) - lse), 0.0)
            p_out[here, keys] = p.astype(jnp.bfloat16)
            d_out[here, keys] = (p * (dp - delta)).astype(jnp.bfloat16)


def grads_of(chunk, p_in, d_in, qdo_t, keys, acc, dq):
    nk = tiles_of(chunk) * TILE
    rows = slice(chunk * CHUNK, (chunk + 1) * CHUNK)
    acc[1, :, :nk] += jnp.dot(qdo_t[HD:, rows], p_in[:, :nk], preferred_element_type=jnp.float32)
    acc[0, :, :nk] += jnp.dot(qdo_t[:HD, rows], d_in[:, :nk], preferred_element_type=jnp.float32)
    dq[rows, :] += jnp.dot(d_in[:, :nk], keys[:nk, :], preferred_element_type=jnp.float32)


def kernel(
    n_blk,
    pos_in,
    start_in,
    q_hbm,
    do_hbm,
    o_hbm,
    k_hbm,
    v_hbm,
    lse_hbm,
    pos_hbm,
    dq_out,
    dk_out,
    dv_out,
    pos_smem,
    start_smem,
    qdo,
    o_buf,
    lse_in,
    kv,
    pos,
    qdo_t,
    lse_b,
    delta_b,
    start_b,
    place_b,
    weights,
    sdp_a,
    sdp_b,
    p_a,
    p_b,
    d_a,
    d_b,
    acc,
    own,
    dq,
    grad_low,
    part,
    inbox,
    mate_box,
    load_sem,
    kv_send,
    kv_recv,
    pos_send,
    pos_recv,
    part_send,
    part_recv,
    mate_recv,
    last_sem,
):
    blk, head = lax.axis_index("blk"), lax.axis_index("head")
    odd = lax.rem(blk, 2) == 1
    even = jnp.logical_not(odd)

    reach = jnp.where(odd, 2, 3)

    def device(shift, across=0):
        return (lax.rem(blk + shift + n_blk, n_blk), lax.rem(head + across, 2))

    barrier = pltpu.get_barrier_semaphore()

    def greet(*where):
        for shift, across in where:
            pl.semaphore_signal(
                barrier, inc=1, device_id=device(shift, across), device_id_type=MESH
            )

    @pl.when(odd)
    def _():
        greet((1, 0), (2, 0), (3, 0), (-1, 0), (-2, 0), (-2, 1), (0, 1))

    @pl.when(even)
    def _():
        greet((1, 0), (-2, 0), (-2, 1), (-3, 0), (-3, 1), (0, 1))

    loads = [
        pltpu.make_async_copy(k_hbm, kv.at[0, 0:TOK, :], load_sem.at[0]),
        pltpu.make_async_copy(v_hbm, kv.at[0, TOK : 2 * TOK, :], load_sem.at[1]),
        pltpu.make_async_copy(pos_hbm, pos.at[0], load_sem.at[2]),
        pltpu.make_async_copy(pos_in, pos_smem, load_sem.at[7]),
        pltpu.make_async_copy(start_in, start_smem, load_sem.at[8]),
        pltpu.make_async_copy(lse_hbm, lse_in, load_sem.at[3]),
        pltpu.make_async_copy(do_hbm, qdo.at[:, HD : 2 * HD], load_sem.at[4]),
        pltpu.make_async_copy(q_hbm, qdo.at[:, 0:HD], load_sem.at[5]),
        pltpu.make_async_copy(o_hbm, o_buf, load_sem.at[6]),
    ]
    for load in loads:
        load.start()

    def kv_copy(src, dst, send, shift):
        to = device(shift)
        return (
            pltpu.make_async_remote_copy(
                kv.at[src], kv.at[dst], kv_send.at[send], kv_recv.at[dst], to, MESH
            ),
            pltpu.make_async_remote_copy(
                pos.at[src], pos.at[dst], pos_send.at[send], pos_recv.at[dst], to, MESH
            ),
        )

    def start_kv(*args):
        for copy in kv_copy(*args):
            copy.start()

    def wait_kv_send(*args):
        for copy in kv_copy(*args):
            copy.wait_send()

    def wait_kv(slot):
        for copy in kv_copy(slot, slot, 0, 0):
            copy.wait_recv()

    def part_copy(src, dst, shift, across=0):
        return pltpu.make_async_remote_copy(
            part.at[src, lax.rem(head + across, 2)],
            inbox.at[dst],
            part_send.at[src, across],
            part_recv.at[dst],
            device(shift, across),
            MESH,
        )

    def mate_copy(src, dst, shift):
        return pltpu.make_async_remote_copy(
            part.at[src],
            mate_box.at[dst],
            part_send.at[src, 0],
            mate_recv.at[dst],
            device(shift),
            MESH,
        )

    def wait_part(dst):
        part_copy(0, dst, 0).wait_recv()

    def wait_mate(dst):
        mate_copy(0, dst, 0).wait_recv()

    def send_halves(src, dst, shift):
        part_copy(src, dst, shift).start()
        part_copy(src, dst + 1, shift, 1).start()

    def low(x):
        return x.astype(jnp.bfloat16)

    def full(x):
        return x.astype(jnp.float32)

    @pl.when(even)
    def _():
        for load in loads[:3]:
            load.wait()
        pl.semaphore_wait(barrier, 6)
        start_kv(0, 1, 0, -1)

    def spread(t, carry):
        at = pl.multiple_of(t * HEADS, HEADS)
        start_b[pl.ds(at, HEADS), :] = jnp.full((HEADS, TILE), start_smem[t], jnp.int32)
        place_b[pl.ds(at, HEADS), :] = jnp.full((HEADS, TILE), pos_smem[t], jnp.int32)
        return carry

    loads[3].wait()
    loads[4].wait()
    lax.fori_loop(0, TOK, spread, 0, unroll=16)
    weights[...] = jnp.zeros_like(weights)
    loads[5].wait()
    lse_t = lse_in[...] * EXP2
    for t in range(TOK):
        lse_b[t * HEADS : (t + 1) * HEADS, :] = jnp.broadcast_to(
            lse_t[:, t : t + 1], (HEADS, TILE)
        )
    @pl.when(odd)
    def _():
        for load in loads[:3]:
            load.wait()
        pl.semaphore_wait(barrier, 7)
        start_kv(0, 1, 0, -1)

    for load in loads[6:]:
        load.wait()

    def prepare(i, carry):
        rows = pl.ds(pl.multiple_of(i * 512, 512), 512)
        grad = qdo[rows, HD:]
        delta = jnp.sum(
            grad.astype(jnp.float32) * o_buf[rows, :].astype(jnp.float32), axis=1, keepdims=True
        )
        delta_b[rows, :] = jnp.broadcast_to(delta, (512, TILE))
        qdo_t[HD:, rows] = jnp.swapaxes(grad, 0, 1)
        qdo_t[:HD, rows] = jnp.swapaxes(qdo[rows, :HD], 0, 1)
        return carry

    lax.fori_loop(0, ROWS // 512, prepare, 0)
    dq[...] = jnp.zeros_like(dq)
    start_kv(0, reach, 1, -reach)

    def work(slot):
        keys = kv.at[slot, 0:TOK, :]
        values = kv.at[slot, TOK : 2 * TOK, :]
        key_pos = pos[slot]
        for j in range(TOK // TILE):
            rows = slice(j * TILE, (j + 1) * TILE)
            at = 2 * j * TILE
            weights[:HD, at : at + TILE] = jnp.swapaxes(keys[rows, :], 0, 1)
            weights[HD:, at + TILE : at + 2 * TILE] = jnp.swapaxes(values[rows, :], 0, 1)
        acc[...] = jnp.zeros_like(acc)
        sdp, p_bf, d_bf = (sdp_a, sdp_b), (p_a, p_b), (d_a, d_b)
        for c in range(-1, N_CHUNK + 1):
            if c + 1 < N_CHUNK:
                scores_of(c + 1, qdo, weights, sdp[(c + 1) % 2])
            if 0 <= c < N_CHUNK:
                attend_of(
                    c, sdp[c % 2], lse_b, delta_b, start_b, place_b, key_pos, p_bf[c % 2], d_bf[c % 2]
                )
            if c >= 1:
                grads_of(c - 1, p_bf[(c - 1) % 2], d_bf[(c - 1) % 2], qdo_t, keys, acc, dq)

    def step(turn, carry):
        slot = jnp.where(jnp.logical_and(odd, turn > 1), 5 - turn, turn)

        @pl.when(turn == 1)
        def _():
            wait_kv(1)

        @pl.when(jnp.logical_and(turn == 1, odd))
        def _():
            start_kv(1, 2, 2, -1)

        @pl.when(jnp.logical_and(turn == 2, odd))
        def _():
            wait_kv(2)
            start_kv(2, 3, 3, -1)
            wait_kv(3)

        @pl.when(jnp.logical_and(turn == 2, even))
        def _():
            wait_kv(2)

        @pl.when(jnp.logical_and(turn == 3, even))
        def _():
            wait_kv(3)

        @pl.when(jnp.logical_and(turn == 3, odd))
        def _():
            wait_mate(BESIDE)
            own[...] += full(mate_box[BESIDE])
            part[3] = low(own[...])
            part_copy(3, TWIN, 0, 1).start()

        work(slot)

        @pl.when(turn == 0)
        def _():
            own[...] = acc[...]

        @pl.when(jnp.logical_and(turn == 0, even))
        def _():
            part[3] = low(own[...])
            part_copy(3, TWIN, 0, 1).start()

        @pl.when(turn == 1)
        def _():
            part[0] = low(acc[...])

        @pl.when(jnp.logical_and(turn == 1, odd))
        def _():
            mate_copy(0, MATE, -1).start()

        @pl.when(jnp.logical_and(turn == 1, even))
        def _():
            mate_copy(0, BESIDE, 1).start()

        @pl.when(jnp.logical_and(turn == 2, odd))
        def _():
            part[1] = low(acc[...])
            send_halves(1, FAR, 3)

        @pl.when(jnp.logical_and(turn == 2, even))
        def _():
            wait_mate(MATE)
            part[1] = low(acc[...] + full(mate_box[MATE]))
            send_halves(1, NEAR, 2)

        @pl.when(jnp.logical_and(turn == 3, odd))
        def _():
            wait_mate(MATE)
            part[2] = low(acc[...] + full(mate_box[MATE]))
            send_halves(2, FAR, 2)

        @pl.when(jnp.logical_and(turn == 3, even))
        def _():
            part[2] = low(acc[...])
            mate_copy(2, MATE, 1).start()

        return carry

    lax.fori_loop(0, STEPS, step, 0)

    for i in range(N_CHUNK):
        rows = slice(i * CHUNK, (i + 1) * CHUNK)
        dq_out[rows, :] = (dq[rows, :] * (SCALE * HALF)).astype(jnp.bfloat16)

    wait_part(TWIN)
    half = own.at[head]
    half[...] += full(inbox[TWIN])

    @pl.when(even)
    def _():
        wait_part(NEAR)
        wait_part(NEAR + 1)
        half[...] += full(inbox[NEAR]) + full(inbox[NEAR + 1])

    wait_part(FAR)
    wait_part(FAR + 1)
    total = half[...] + (full(inbox[FAR]) + full(inbox[FAR + 1]))
    factor = jnp.where(head == 0, SCALE * HALF, HALF)
    grad_low[head] = low(jnp.swapaxes(total * factor, 0, 1))
    last = pltpu.make_async_remote_copy(
        grad_low.at[head], grad_low.at[head], last_sem.at[0], last_sem.at[1], device(0, 1), MESH
    )
    last.start()
    last.wait()
    dk_out[...] = grad_low[0]
    dv_out[...] = grad_low[1]

    def sent(src, dst, shift, across=0):
        part_copy(src, dst, shift, across).wait_send()

    sent(3, TWIN, 0, 1)
    wait_kv_send(0, 1, 0, -1)
    wait_kv_send(0, reach, 1, -reach)

    @pl.when(odd)
    def _():
        wait_kv_send(1, 2, 2, -1)
        wait_kv_send(2, 3, 3, -1)
        mate_copy(0, MATE, -1).wait_send()
        sent(1, FAR, 3)
        sent(1, FAR + 1, 3, 1)
        sent(2, FAR, 2)
        sent(2, FAR + 1, 2, 1)

    @pl.when(even)
    def _():
        mate_copy(0, BESIDE, 1).wait_send()
        sent(1, NEAR, 2)
        sent(1, NEAR + 1, 2, 1)
        mate_copy(2, MATE, 1).wait_send()


def call(n_blk, q, do, o, k, v, lse, pos, start):
    in_hbm = pl.BlockSpec(memory_space=pltpu.HBM)
    flat = (ROWS, HD)
    low, full = jnp.bfloat16, jnp.float32
    dq, dk, dv = pl.pallas_call(
        functools.partial(kernel, n_blk),
        out_shape=(
            pltpu.VMEM(flat, low),
            pltpu.VMEM(k.shape, low),
            pltpu.VMEM(v.shape, low),
        ),
        in_specs=[in_hbm] * 9,
        out_specs=(pl.BlockSpec(memory_space=pltpu.VMEM),) * 3,
        scratch_shapes=[
            pltpu.SMEM((TOK,), jnp.int32),
            pltpu.SMEM((TOK,), jnp.int32),
            pltpu.VMEM((ROWS, 2 * HD), low),
            pltpu.VMEM(flat, low),
            pltpu.VMEM((HEADS, TOK), full),
            pltpu.VMEM((STEPS, 2 * TOK, HD), low),
            pltpu.VMEM((STEPS, TOK // TILE, TILE), jnp.int32),
            pltpu.VMEM((2 * HD, ROWS), low),
            pltpu.VMEM(flat, full),
            pltpu.VMEM(flat, full),
            pltpu.VMEM(flat, jnp.int32),
            pltpu.VMEM(flat, jnp.int32),
            pltpu.VMEM((2 * HD, 2 * TOK), low),
            pltpu.VMEM((CHUNK, 2 * TOK), full),
            pltpu.VMEM((CHUNK, 2 * TOK), full),
            pltpu.VMEM((CHUNK, TOK), low),
            pltpu.VMEM((CHUNK, TOK), low),
            pltpu.VMEM((CHUNK, TOK), low),
            pltpu.VMEM((CHUNK, TOK), low),
            pltpu.VMEM((2, HD, TOK), full),
            pltpu.VMEM((2, HD, TOK), full),
            pltpu.VMEM(flat, full),
            pltpu.VMEM((2, TOK, HD), low),
            pltpu.VMEM((4, 2, HD, TOK), low),
            pltpu.VMEM((5, HD, TOK), low),
            pltpu.VMEM((2, 2, HD, TOK), low),
            pltpu.SemaphoreType.DMA((9,)),
            pltpu.SemaphoreType.DMA((4,)),
            pltpu.SemaphoreType.DMA((4,)),
            pltpu.SemaphoreType.DMA((4,)),
            pltpu.SemaphoreType.DMA((4,)),
            pltpu.SemaphoreType.DMA((4, 2)),
            pltpu.SemaphoreType.DMA((5,)),
            pltpu.SemaphoreType.DMA((2,)),
            pltpu.SemaphoreType.DMA((2,)),
        ],
        compiler_params=pltpu.CompilerParams(
            collective_id=0,
            has_side_effects=True,
            vmem_limit_bytes=125 * 512 * 1024,
        ),
    )(
        pos,
        start,
        q.reshape(flat),
        do.reshape(flat),
        o.reshape(flat),
        k,
        v,
        lse.T,
        pos.reshape(TOK // TILE, TILE),
    )
    return dq.reshape(q.shape) * 2, dk * 2, dv * 2


def solution(mesh):
    n_blk = mesh.shape["blk"]
    in_specs = (
        P("blk", "head", None),
        P("blk", "head", None),
        P("blk", "head", None),
        P("blk", None),
        P("blk", None),
        P("blk", "head"),
        P("blk"),
        P("blk"),
    )
    out_specs = (P("blk", "head", None), P("blk", None), P("blk", None))
    return jax.shard_map(
        functools.partial(call, n_blk),
        mesh=mesh,
        in_specs=in_specs,
        out_specs=out_specs,
        check_vma=False,
    )
```

```python
import functools
import math

import jax
import jax.numpy as jnp
from jax import lax
from jax.experimental import pallas as pl
from jax.experimental.pallas import tpu as pltpu
from jax.sharding import PartitionSpec as P

MESH = pl.DeviceIdType.MESH
STEPS = 4
TOK = 512
HEADS = 8
HD = 128
ROWS = TOK * HEADS
CHUNK = 512
N_CHUNK = ROWS // CHUNK
TILE = 128
EXP2 = math.log2(math.e)
SCALE = HD**-0.5
HALF = 0.5
MATE, BESIDE = 0, 1
NEAR, FAR, TWIN = 0, 2, 4


def tiles_of(chunk):
    last = (chunk + 1) * CHUNK // HEADS
    return -(-last // TILE)


def scores_of(chunk, qdo, weights, sdp):
    width = 2 * TILE * tiles_of(chunk)
    sdp[:, :width] = jnp.dot(
        qdo[chunk * CHUNK : (chunk + 1) * CHUNK, :],
        weights[:, :width],
        preferred_element_type=jnp.float32,
    )


def attend_of(chunk, sdp, lse_b, delta_b, start_b, place_b, key_pos, p_out, d_out):
    piece = 64
    for at in range(0, CHUNK, piece):
        here = slice(at, at + piece)
        rows = slice(chunk * CHUNK + at, chunk * CHUNK + at + piece)
        lse, delta = lse_b[rows, :], delta_b[rows, :]
        start = start_b[rows, :]
        for j in range(tiles_of(chunk)):
            keys = slice(j * TILE, (j + 1) * TILE)
            s = sdp[here, 2 * j * TILE : (2 * j + 1) * TILE]
            dp = sdp[here, (2 * j + 1) * TILE : (2 * j + 2) * TILE]
            at_key = key_pos[j : j + 1, :]
            met = at_key >= start
            if (j + 1) * TILE * HEADS > chunk * CHUNK:
                met = jnp.logical_and(met, at_key <= place_b[rows, :])
            p = jnp.where(met, jnp.exp2(s * (SCALE * EXP2) - lse), 0.0)
            p_out[here, keys] = p.astype(jnp.bfloat16)
            d_out[here, keys] = (p * (dp - delta)).astype(jnp.bfloat16)


def grads_of(chunk, p_in, d_in, qdo_t, keys, acc, dq):
    nk = tiles_of(chunk) * TILE
    rows = slice(chunk * CHUNK, (chunk + 1) * CHUNK)
    acc[1, :, :nk] += jnp.dot(qdo_t[HD:, rows], p_in[:, :nk], preferred_element_type=jnp.float32)
    acc[0, :, :nk] += jnp.dot(qdo_t[:HD, rows], d_in[:, :nk], preferred_element_type=jnp.float32)
    dq[rows, :] += jnp.dot(d_in[:, :nk], keys[:nk, :], preferred_element_type=jnp.float32)


def kernel(
    n_blk,
    pos_in,
    start_in,
    q_hbm,
    do_hbm,
    o_hbm,
    k_hbm,
    v_hbm,
    lse_hbm,
    pos_hbm,
    dq_out,
    dk_out,
    dv_out,
    pos_smem,
    start_smem,
    qdo,
    o_buf,
    lse_in,
    kv,
    pos,
    qdo_t,
    lse_b,
    delta_b,
    start_b,
    place_b,
    weights,
    sdp_a,
    sdp_b,
    p_a,
    p_b,
    d_a,
    d_b,
    acc,
    own,
    dq,
    grad_low,
    part,
    inbox,
    mate_box,
    load_sem,
    kv_send,
    kv_recv,
    pos_send,
    pos_recv,
    part_send,
    part_recv,
    mate_recv,
    last_sem,
    far_send,
    far_recv,
):
    blk, head = lax.axis_index("blk"), lax.axis_index("head")
    odd = lax.rem(blk, 2) == 1
    even = jnp.logical_not(odd)

    reach = jnp.where(odd, 2, 3)

    def device(shift, across=0):
        return (lax.rem(blk + shift + n_blk, n_blk), lax.rem(head + across, 2))

    barrier = pltpu.get_barrier_semaphore()

    def greet(*where):
        for shift, across in where:
            pl.semaphore_signal(
                barrier, inc=1, device_id=device(shift, across), device_id_type=MESH
            )

    @pl.when(odd)
    def _():
        greet((1, 0), (2, 0), (3, 0), (-1, 0), (-2, 0), (-2, 1), (0, 1))

    @pl.when(even)
    def _():
        greet((1, 0), (-2, 0), (-2, 1), (-3, 0), (-3, 1), (0, 1))

    loads = [
        pltpu.make_async_copy(k_hbm, kv.at[0, 0:TOK, :], load_sem.at[0]),
        pltpu.make_async_copy(v_hbm, kv.at[0, TOK : 2 * TOK, :], load_sem.at[1]),
        pltpu.make_async_copy(pos_hbm, pos.at[0], load_sem.at[2]),
        pltpu.make_async_copy(pos_in, pos_smem, load_sem.at[7]),
        pltpu.make_async_copy(start_in, start_smem, load_sem.at[8]),
        pltpu.make_async_copy(lse_hbm, lse_in, load_sem.at[3]),
        pltpu.make_async_copy(do_hbm, qdo.at[:, HD : 2 * HD], load_sem.at[4]),
        pltpu.make_async_copy(q_hbm, qdo.at[:, 0:HD], load_sem.at[5]),
        pltpu.make_async_copy(o_hbm, o_buf, load_sem.at[6]),
    ]
    for load in loads:
        load.start()

    def kv_copy(src, dst, send, shift):
        to = device(shift)
        return (
            pltpu.make_async_remote_copy(
                kv.at[src], kv.at[dst], kv_send.at[send], kv_recv.at[dst], to, MESH
            ),
            pltpu.make_async_remote_copy(
                pos.at[src], pos.at[dst], pos_send.at[send], pos_recv.at[dst], to, MESH
            ),
        )

    def start_kv(*args):
        for copy in kv_copy(*args):
            copy.start()

    def wait_kv_send(*args):
        for copy in kv_copy(*args):
            copy.wait_send()

    def wait_kv(slot):
        for copy in kv_copy(slot, slot, 0, 0):
            copy.wait_recv()

    def part_copy(src, dst, shift, across=0):
        return pltpu.make_async_remote_copy(
            part.at[src, lax.rem(head + across, 2)],
            inbox.at[dst],
            part_send.at[src, across],
            part_recv.at[dst],
            device(shift, across),
            MESH,
        )

    def mate_copy(src, dst, shift):
        return pltpu.make_async_remote_copy(
            part.at[src],
            mate_box.at[dst],
            part_send.at[src, 0],
            mate_recv.at[dst],
            device(shift),
            MESH,
        )

    pieces = [slice(0, TOK // 2), slice(TOK // 2, TOK)]

    def far_copy(src, shift, across, i):
        return pltpu.make_async_remote_copy(
            part.at[src, lax.rem(head + across, 2), :, pieces[i]],
            inbox.at[FAR + across, :, pieces[i]],
            far_send.at[src - 1, across, i],
            far_recv.at[across, i],
            device(shift, across),
            MESH,
        )

    def each_far(src, shift):
        return [far_copy(src, shift, across, i) for i in range(2) for across in range(2)]

    def wait_part(dst):
        part_copy(0, dst, 0).wait_recv()

    def wait_mate(dst):
        mate_copy(0, dst, 0).wait_recv()

    def send_halves(src, dst, shift):
        part_copy(src, dst, shift).start()
        part_copy(src, dst + 1, shift, 1).start()

    def low(x):
        return x.astype(jnp.bfloat16)

    def full(x):
        return x.astype(jnp.float32)

    @pl.when(even)
    def _():
        for load in loads[:3]:
            load.wait()
        pl.semaphore_wait(barrier, 6)
        start_kv(0, 1, 0, -1)

    def spread(t, carry):
        at = pl.multiple_of(t * HEADS, HEADS)
        start_b[pl.ds(at, HEADS), :] = jnp.full((HEADS, TILE), start_smem[t], jnp.int32)
        place_b[pl.ds(at, HEADS), :] = jnp.full((HEADS, TILE), pos_smem[t], jnp.int32)
        return carry

    loads[3].wait()
    loads[4].wait()
    lax.fori_loop(0, TOK, spread, 0, unroll=16)
    weights[...] = jnp.zeros_like(weights)
    loads[5].wait()
    lse_t = lse_in[...] * EXP2
    for t in range(TOK):
        lse_b[t * HEADS : (t + 1) * HEADS, :] = jnp.broadcast_to(
            lse_t[:, t : t + 1], (HEADS, TILE)
        )
    @pl.when(odd)
    def _():
        for load in loads[:3]:
            load.wait()
        pl.semaphore_wait(barrier, 7)
        start_kv(0, 1, 0, -1)

    for load in loads[6:]:
        load.wait()

    def prepare(i, carry):
        rows = pl.ds(pl.multiple_of(i * 512, 512), 512)
        grad = qdo[rows, HD:]
        delta = jnp.sum(
            grad.astype(jnp.float32) * o_buf[rows, :].astype(jnp.float32), axis=1, keepdims=True
        )
        delta_b[rows, :] = jnp.broadcast_to(delta, (512, TILE))
        qdo_t[HD:, rows] = jnp.swapaxes(grad, 0, 1)
        qdo_t[:HD, rows] = jnp.swapaxes(qdo[rows, :HD], 0, 1)
        return carry

    lax.fori_loop(0, ROWS // 512, prepare, 0)
    dq[...] = jnp.zeros_like(dq)
    start_kv(0, reach, 1, -reach)

    def work(slot):
        keys = kv.at[slot, 0:TOK, :]
        values = kv.at[slot, TOK : 2 * TOK, :]
        key_pos = pos[slot]
        for j in range(TOK // TILE):
            rows = slice(j * TILE, (j + 1) * TILE)
            at = 2 * j * TILE
            weights[:HD, at : at + TILE] = jnp.swapaxes(keys[rows, :], 0, 1)
            weights[HD:, at + TILE : at + 2 * TILE] = jnp.swapaxes(values[rows, :], 0, 1)
        acc[...] = jnp.zeros_like(acc)
        sdp, p_bf, d_bf = (sdp_a, sdp_b), (p_a, p_b), (d_a, d_b)
        for c in range(-1, N_CHUNK + 1):
            if c + 1 < N_CHUNK:
                scores_of(c + 1, qdo, weights, sdp[(c + 1) % 2])
            if 0 <= c < N_CHUNK:
                attend_of(
                    c, sdp[c % 2], lse_b, delta_b, start_b, place_b, key_pos, p_bf[c % 2], d_bf[c % 2]
                )
            if c >= 1:
                grads_of(c - 1, p_bf[(c - 1) % 2], d_bf[(c - 1) % 2], qdo_t, keys, acc, dq)

    def step(turn, carry):
        slot = jnp.where(jnp.logical_and(odd, turn > 1), 5 - turn, turn)

        @pl.when(turn == 1)
        def _():
            wait_kv(1)

        @pl.when(jnp.logical_and(turn == 1, odd))
        def _():
            start_kv(1, 2, 2, -1)

        @pl.when(jnp.logical_and(turn == 2, odd))
        def _():
            wait_kv(2)
            start_kv(2, 3, 3, -1)
            wait_kv(3)

        @pl.when(jnp.logical_and(turn == 2, even))
        def _():
            wait_kv(2)

        @pl.when(jnp.logical_and(turn == 3, even))
        def _():
            wait_kv(3)

        @pl.when(jnp.logical_and(turn == 3, odd))
        def _():
            wait_mate(BESIDE)
            own[...] += full(mate_box[BESIDE])
            part[3] = low(own[...])
            part_copy(3, TWIN, 0, 1).start()

        work(slot)

        @pl.when(turn == 0)
        def _():
            own[...] = acc[...]

        @pl.when(jnp.logical_and(turn == 0, even))
        def _():
            part[3] = low(own[...])
            part_copy(3, TWIN, 0, 1).start()

        @pl.when(turn == 1)
        def _():
            part[0] = low(acc[...])

        @pl.when(jnp.logical_and(turn == 1, odd))
        def _():
            mate_copy(0, MATE, -1).start()

        @pl.when(jnp.logical_and(turn == 1, even))
        def _():
            mate_copy(0, BESIDE, 1).start()

        @pl.when(jnp.logical_and(turn == 2, odd))
        def _():
            part[1] = low(acc[...])
            for copy in each_far(1, 3):
                copy.start()

        @pl.when(jnp.logical_and(turn == 2, even))
        def _():
            wait_mate(MATE)
            part[1] = low(acc[...] + full(mate_box[MATE]))
            send_halves(1, NEAR, 2)

        @pl.when(jnp.logical_and(turn == 3, odd))
        def _():
            wait_mate(MATE)
            part[2] = low(acc[...] + full(mate_box[MATE]))
            for copy in each_far(2, 2):
                copy.start()

        @pl.when(jnp.logical_and(turn == 3, even))
        def _():
            part[2] = low(acc[...])
            mate_copy(2, MATE, 1).start()

        return carry

    lax.fori_loop(0, STEPS, step, 0)

    for i in range(N_CHUNK):
        rows = slice(i * CHUNK, (i + 1) * CHUNK)
        dq_out[rows, :] = (dq[rows, :] * (SCALE * HALF)).astype(jnp.bfloat16)

    wait_part(TWIN)
    half = own.at[head]
    half[...] += full(inbox[TWIN])

    @pl.when(even)
    def _():
        wait_part(NEAR)
        wait_part(NEAR + 1)
        half[...] += full(inbox[NEAR]) + full(inbox[NEAR + 1])

    factor = jnp.where(head == 0, SCALE * HALF, HALF)
    lasts = []
    for i, keys in enumerate(pieces):
        for across in range(2):
            far_copy(1, 0, across, i).wait_recv()
        total = half[:, keys] + (full(inbox[FAR, :, keys]) + full(inbox[FAR + 1, :, keys]))
        grad_low[head, keys, :] = low(jnp.swapaxes(total * factor, 0, 1))
        lasts.append(
            pltpu.make_async_remote_copy(
                grad_low.at[head, keys],
                grad_low.at[head, keys],
                last_sem.at[0, i],
                last_sem.at[1, i],
                device(0, 1),
                MESH,
            )
        )
        lasts[i].start()
    for last in lasts:
        last.wait()
    dk_out[...] = grad_low[0]
    dv_out[...] = grad_low[1]

    def sent(src, dst, shift, across=0):
        part_copy(src, dst, shift, across).wait_send()

    sent(3, TWIN, 0, 1)
    wait_kv_send(0, 1, 0, -1)
    wait_kv_send(0, reach, 1, -reach)

    @pl.when(odd)
    def _():
        wait_kv_send(1, 2, 2, -1)
        wait_kv_send(2, 3, 3, -1)
        mate_copy(0, MATE, -1).wait_send()
        for copy in each_far(1, 3) + each_far(2, 2):
            copy.wait_send()

    @pl.when(even)
    def _():
        mate_copy(0, BESIDE, 1).wait_send()
        sent(1, NEAR, 2)
        sent(1, NEAR + 1, 2, 1)
        mate_copy(2, MATE, 1).wait_send()


def call(n_blk, q, do, o, k, v, lse, pos, start):
    in_hbm = pl.BlockSpec(memory_space=pltpu.HBM)
    flat = (ROWS, HD)
    low, full = jnp.bfloat16, jnp.float32
    dq, dk, dv = pl.pallas_call(
        functools.partial(kernel, n_blk),
        out_shape=(
            pltpu.VMEM(flat, low),
            pltpu.VMEM(k.shape, low),
            pltpu.VMEM(v.shape, low),
        ),
        in_specs=[in_hbm] * 9,
        out_specs=(pl.BlockSpec(memory_space=pltpu.VMEM),) * 3,
        scratch_shapes=[
            pltpu.SMEM((TOK,), jnp.int32),
            pltpu.SMEM((TOK,), jnp.int32),
            pltpu.VMEM((ROWS, 2 * HD), low),
            pltpu.VMEM(flat, low),
            pltpu.VMEM((HEADS, TOK), full),
            pltpu.VMEM((STEPS, 2 * TOK, HD), low),
            pltpu.VMEM((STEPS, TOK // TILE, TILE), jnp.int32),
            pltpu.VMEM((2 * HD, ROWS), low),
            pltpu.VMEM(flat, full),
            pltpu.VMEM(flat, full),
            pltpu.VMEM(flat, jnp.int32),
            pltpu.VMEM(flat, jnp.int32),
            pltpu.VMEM((2 * HD, 2 * TOK), low),
            pltpu.VMEM((CHUNK, 2 * TOK), full),
            pltpu.VMEM((CHUNK, 2 * TOK), full),
            pltpu.VMEM((CHUNK, TOK), low),
            pltpu.VMEM((CHUNK, TOK), low),
            pltpu.VMEM((CHUNK, TOK), low),
            pltpu.VMEM((CHUNK, TOK), low),
            pltpu.VMEM((2, HD, TOK), full),
            pltpu.VMEM((2, HD, TOK), full),
            pltpu.VMEM(flat, full),
            pltpu.VMEM((2, TOK, HD), low),
            pltpu.VMEM((4, 2, HD, TOK), low),
            pltpu.VMEM((5, HD, TOK), low),
            pltpu.VMEM((2, 2, HD, TOK), low),
            pltpu.SemaphoreType.DMA((9,)),
            pltpu.SemaphoreType.DMA((4,)),
            pltpu.SemaphoreType.DMA((4,)),
            pltpu.SemaphoreType.DMA((4,)),
            pltpu.SemaphoreType.DMA((4,)),
            pltpu.SemaphoreType.DMA((4, 2)),
            pltpu.SemaphoreType.DMA((5,)),
            pltpu.SemaphoreType.DMA((2,)),
            pltpu.SemaphoreType.DMA((2, 2)),
            pltpu.SemaphoreType.DMA((2, 2, 2)),
            pltpu.SemaphoreType.DMA((2, 2)),
        ],
        compiler_params=pltpu.CompilerParams(
            collective_id=0,
            has_side_effects=True,
            vmem_limit_bytes=125 * 512 * 1024,
        ),
    )(
        pos,
        start,
        q.reshape(flat),
        do.reshape(flat),
        o.reshape(flat),
        k,
        v,
        lse.T,
        pos.reshape(TOK // TILE, TILE),
    )
    return dq.reshape(q.shape) * 2, dk * 2, dv * 2


def solution(mesh):
    n_blk = mesh.shape["blk"]
    in_specs = (
        P("blk", "head", None),
        P("blk", "head", None),
        P("blk", "head", None),
        P("blk", None),
        P("blk", None),
        P("blk", "head"),
        P("blk"),
        P("blk"),
    )
    out_specs = (P("blk", "head", None), P("blk", None), P("blk", None))
    return jax.shard_map(
        functools.partial(call, n_blk),
        mesh=mesh,
        in_specs=in_specs,
        out_specs=out_specs,
        check_vma=False,
    )
```
